16 devices in a mesh: dp: 2 (over y, z), tp: 8 (over x, core).
Axes of the slice: x: 4, y: 2, z: 1, core: 2. Of those that a mesh axis runs over, the one named last changes fastest.
The devices are a block of a 4x4x8 slice.
Arguments:
- x_saved: bfloat16 [2, 16384, 1536], P(None, ('dp', 'tp')), parts along dimension 1
- pre_act: bfloat16 [2, 16384, 6144], P(None, 'dp', 'tp'), parts along dimension 1
- w_in: bfloat16 [1536, 6144], P(None, 'tp')
- w_out: bfloat16 [6144, 1536], P('tp')
- grad_out: bfloat16 [2, 16384, 1536], P(None, ('dp', 'tp')), parts along dimension 1
Outputs:
- output 1: bfloat16 [2, 16384, 1536], P(None, ('dp', 'tp')), parts along dimension 1
- output 2: float32 [3072, 6144], P('dp', 'tp'), parts along dimension 0
- output 3: float32 [12288, 1536], P(('dp', 'tp')), parts along dimension 0
There are 2 independent parts. The reference program is written for one: setup_inputs(seed, part) draws one part's arguments, and reference() takes and returns one part's arrays. A program takes and returns all parts, laid end to end along the dimension named above; an argument that names none is the same for every part.
All inputs are finite; a program needn't handle non-finite values.
Results may differ from the reference program's by a relative error of at most 0.001.
Values are sent between devices in bfloat16 or wider.
A program may use at most 768 MiB of HBM per device.

```python
import jax
import jax.numpy as jnp
from jax import lax

MICRO_BATCHES = 2
TOKENS = 8192
HIDDEN = 1536
FFN_DIM = 6144


def gelu_tanh(values):
    return jax.nn.gelu(values, approximate=True)


def setup_inputs(seed: int = 0, part: int = 0) -> dict:
    part_key = jax.random.fold_in(jax.random.key(seed), part)
    key_x, key_u, key_dy = jax.random.split(part_key, 3)
    key_w1, key_w2 = jax.random.split(jax.random.key(seed + 7919), 2)
    x_saved = jax.random.normal(key_x, (MICRO_BATCHES, TOKENS, HIDDEN), jnp.float32).astype(jnp.bfloat16)
    pre_act = jax.random.normal(key_u, (MICRO_BATCHES, TOKENS, FFN_DIM), jnp.float32).astype(jnp.bfloat16)
    w_in = (jax.random.normal(key_w1, (HIDDEN, FFN_DIM), jnp.float32) * HIDDEN ** -0.5).astype(jnp.bfloat16)
    w_out = (jax.random.normal(key_w2, (FFN_DIM, HIDDEN), jnp.float32) * FFN_DIM ** -0.5).astype(jnp.bfloat16)
    grad_out = jax.random.normal(key_dy, (MICRO_BATCHES, TOKENS, HIDDEN), jnp.float32).astype(jnp.bfloat16)
    return {'x_saved': x_saved, 'pre_act': pre_act, 'w_in': w_in, 'w_out': w_out, 'grad_out': grad_out}


def reference(x_saved, pre_act, w_in, w_out, grad_out):
    def one_micro(operands):
        x_rows, pre_rows, dy_rows = operands
        activation, gelu_vjp = jax.vjp(gelu_tanh, pre_rows.astype(jnp.float32))
        act_bf = activation.astype(jnp.bfloat16)
        grad_w_out = jnp.dot(act_bf.T, dy_rows, preferred_element_type=jnp.float32)
        grad_act = jnp.dot(dy_rows, w_out.T, preferred_element_type=jnp.float32)
        grad_pre = gelu_vjp(grad_act)[0].astype(jnp.bfloat16)
        grad_x = jnp.dot(grad_pre, w_in.T, preferred_element_type=jnp.float32).astype(jnp.bfloat16)
        grad_w_in = jnp.dot(x_rows.T, grad_pre, preferred_element_type=jnp.float32)
        return grad_x, grad_w_in, grad_w_out

    grad_x, w_in_parts, w_out_parts = lax.map(one_micro, (x_saved, pre_act, grad_out))
    return grad_x, jnp.sum(w_in_parts, axis=0), jnp.sum(w_out_parts, axis=0)
```

```python
import jax
import jax.numpy as jnp
from jax import lax
from jax.sharding import PartitionSpec as P


def gelu_tanh(values):
    return jax.nn.gelu(values, approximate=True)


def solution(mesh):
    size = mesh.shape['tp']
    chips = size // 2

    def pairs(other):
        return [(d, other(d // 2, d % 2)) for d in range(size)]

    token_pairs = pairs(lambda chip, core: 2 * (chip ^ 1) + core)
    column_pairs = pairs(lambda chip, core: 2 * (chips - 1 - chip) + core)
    core_pairs = pairs(lambda chip, core: 2 * chip + 1 - core)

    def device_backward(x_own, pre_own, w_in_own, w_out_own, dy_own):
        rows = x_own.shape[1]
        me = lax.axis_index('tp')
        chip, core = me // 2, me % 2

        def swap(values, partners):
            return lax.ppermute(values, 'tp', partners)

        def owners(at):
            far = at ^ 1
            return [2 * far + 1 - core, 2 * far + core, 2 * at + 1 - core, 2 * at + core]

        def token_rows(values, owner):
            return lax.dynamic_slice_in_dim(values, owner * rows, rows, axis=1)

        w_out_far = swap(w_out_own, column_pairs)
        dy_far = swap(dy_own, token_pairs)
        dy_side = swap(dy_own, core_pairs)
        pre_far = []
        theirs = owners(chips - 1 - chip)
        pre_far.append(swap(token_rows(pre_own, theirs[0]), column_pairs))
        w_in_far = swap(w_in_own, column_pairs)
        for owner in theirs[1:]:
            pre_far.append(swap(token_rows(pre_own, owner), column_pairs))
        x_far = swap(x_own, token_pairs)
        x_side = swap(x_own, core_pairs)
        dy_far_side = swap(dy_far, core_pairs)
        x_far_side = swap(x_far, core_pairs)
        dys = [dy_far_side, dy_far, dy_side, dy_own]
        xs = [x_far_side, x_far, x_side, x_own]
        mine = owners(chip)

        def step(pre, dy, w_out):
            activation, gelu_vjp = jax.vjp(gelu_tanh, pre.astype(jnp.float32))
            act_bf = activation.astype(jnp.bfloat16)
            grad_act = jnp.einsum('mth,fh->mtf', dy, w_out, preferred_element_type=jnp.float32)
            grad_pre = gelu_vjp(grad_act)[0].astype(jnp.bfloat16)
            grad_w_out = jnp.einsum('mtf,mth->fh', act_bf, dy, preferred_element_type=jnp.float32)
            return grad_pre, grad_w_out

        sums = [[None, None], [None, None]]

        def add(side, which, term):
            old = sums[side][which]
            sums[side][which] = term if old is None else old + term

        parts = []
        for k in range(4):
            near_pre, near_out = step(token_rows(pre_own, mine[k]), dys[k], w_out_own)
            far_pre, far_out = step(pre_far[k], dys[k], w_out_far)
            add(0, 1, near_out)
            add(1, 1, far_out)
            add(0, 0, jnp.einsum('mth,mtf->hf', xs[k], near_pre, preferred_element_type=jnp.float32))
            add(1, 0, jnp.einsum('mth,mtf->hf', xs[k], far_pre, preferred_element_type=jnp.float32))
            part = jnp.einsum('mtf,hf->mth', near_pre, w_in_own, preferred_element_type=jnp.float32)
            part = part + jnp.einsum('mtf,hf->mth', far_pre, w_in_far, preferred_element_type=jnp.float32)
            parts.append(part)

        far_sum = parts[1] + swap(parts[0], core_pairs)
        arrived = swap(far_sum, token_pairs)
        own_sum = parts[3] + swap(parts[2], core_pairs)
        grad_x = (own_sum + arrived).astype(jnp.bfloat16)
        grad_w_out = sums[0][1] + swap(sums[1][1], column_pairs)
        grad_w_in = sums[0][0] + swap(sums[1][0], column_pairs)
        return grad_x, grad_w_in, grad_w_out

    token_spec = P(None, ('dp', 'tp'), None)
    in_specs = (token_spec, P(None, 'dp', 'tp'), P(None, 'tp'), P('tp', None), token_spec)
    out_specs = (token_spec, P('dp', 'tp'), P(('dp', 'tp'), None))
    return jax.shard_map(device_backward, mesh=mesh, in_specs=in_specs, out_specs=out_specs, check_vma=False)
```
